32 devices in a mesh: lat: 4 (over y, x), lon: 8 (over z, core).
Axes of the slice: x: 2, y: 2, z: 4, core: 2. Of those that a mesh axis runs over, the one named last changes fastest.
Arguments:
- latent_field: bfloat16 [640, 32, 64], P(None, 'lat', 'lon'), may hold values from -6 to 6
- spectral_filter: float32 [640, 32], P('lon'), may hold values from -5 to 5
- conv_weight: float32 [9, 640], replicated, may hold values from -2 to 2
- norm_gain: float32 [640], replicated, may hold values from 0.1 to 1.9
- weight_in: bfloat16 [640, 1280], replicated, may hold values from -0.25 to 0.25
- weight_out: bfloat16 [1280, 640], replicated, may hold values from -0.15625 to 0.15625
Outputs:
- updated: bfloat16 [640, 32, 64], P(None, 'lat', 'lon')
The draws below stay inside these ranges and needn't reach their ends.
All inputs are finite; a program needn't handle non-finite values.
Results may differ from the reference program's by a relative error of at most 0.01.
Values may be sent and summed in bfloat16 or wider, within the bound.
A program may use at most 128 MiB of HBM per device.

```python
import math
import jax
import jax.numpy as jnp
from jax import lax

C = 640
HID = 1280
LAT_DEV = 8
NLAT = 32
NLON = 64
N_LAT = 4
N_LON = 8


def steps_of(key, dims, cuts, least, largest):
    gain, own = 1.0, jax.random.fold_in(key, 6)
    for axis_at, parts in cuts:
        steps = jnp.exp(jax.random.uniform(jax.random.fold_in(own, axis_at), (parts,), jnp.float32, least / len(cuts), largest / len(cuts)))
        gain = gain * jnp.repeat(steps, dims[axis_at] // parts).reshape([-1 if axis == axis_at else 1 for axis in range(len(dims))])
    return gain


def scatter_about(own_key, dims, scale, bound, pieces=(), kind=jnp.bfloat16):
    drawn = jax.random.normal(own_key, dims, jnp.float32) * scale
    if len(pieces) > 0:
        drawn = steps_of(own_key, dims, pieces, -0.22, 0.18) * drawn
    return jnp.clip(drawn, min=-bound, max=bound).astype(kind)


def setup_inputs(seed: int = 0) -> dict:
    keys = jax.random.split(jax.random.key(seed), 7)
    return {
        "latent_field": scatter_about(keys[0], (C, NLAT, NLON), 1.0, 6.0, ((1, 4), (2, 8))),
        "spectral_filter": scatter_about(keys[1], (C, NLAT), 1.0, 5.0, ((0, 8),), jnp.float32),
        "conv_weight": scatter_about(keys[2], (9, C), 9 ** -0.5, 2.0, (), jnp.float32),
        "norm_gain": jnp.clip(1.0 + 0.18 * jax.random.normal(keys[3], (C,), jnp.float32), 0.1, 1.9),
        "weight_in": scatter_about(keys[4], (C, HID), C ** -0.5, 0.25),
        "weight_out": scatter_about(keys[5], (HID, C), HID ** -0.5, 0.15625),
    }


highest = lax.Precision.HIGHEST
epsilon_norm = 1e-06

def quadrature(lat_count):
    colatitude = (jnp.arange(lat_count, dtype=jnp.float32) + 0.5) * (math.pi / lat_count)
    return jnp.sin(colatitude) * (math.pi / lat_count)

def fourier_tables(lon_count, mode_count):
    wave_index = jnp.arange(mode_count, dtype=jnp.int32)[:, None] * jnp.arange(lon_count, dtype=jnp.int32)[None, :]
    phase_angle = (wave_index % lon_count).astype(jnp.float32) * (2.0 * math.pi / lon_count)
    cosine = jnp.cos(phase_angle)
    sine_table = jnp.sin(phase_angle)
    angle_step = 2.0 * math.pi / lon_count
    forward = jnp.concatenate([angle_step * cosine, -angle_step * sine_table], axis=0)
    weight = jnp.where(jnp.arange(mode_count, dtype=jnp.int32) == 0, 1.0, 2.0).astype(jnp.float32)[:, None]
    inverse = jnp.concatenate([weight * cosine, -weight * sine_table], axis=0)
    return (forward, inverse)

def legendre_rows(order_ids, lat_count):
    colatitude = (jnp.arange(lat_count, dtype=jnp.float32) + 0.5) * (math.pi / lat_count)
    cosine = jnp.cos(colatitude)
    sine_col = jnp.sin(colatitude)
    order_f = order_ids.astype(jnp.float32)
    factor_index = jnp.arange(1, lat_count, dtype=jnp.float32)
    ratio_log = jnp.log((2.0 * factor_index - 1.0) / (2.0 * factor_index))
    included = (factor_index[None, :] <= order_f[:, None]).astype(jnp.float32)
    log_factor = lax.optimization_barrier(jnp.sum(included * ratio_log[None, :], axis=1))
    start_log = 0.5 * jnp.log((2.0 * order_f + 1.0) / (4.0 * math.pi)) + 0.5 * log_factor
    start_log = start_log[:, None] + order_f[:, None] * jnp.log(sine_col)[None, :]
    blank_rows = jnp.zeros((order_ids.shape[0], lat_count), jnp.float32)
    order_col = order_f[:, None]

    def advance(state_carry, degree):
        before, current, scale_log = state_carry
        degree_f = degree.astype(jnp.float32)
        alpha_term = jnp.sqrt((4.0 * degree_f * degree_f - 1.0) / jnp.maximum(degree_f * degree_f - order_col * order_col, 1.0))
        beta_term = jnp.sqrt(jnp.maximum((degree_f - 1.0) ** 2 - order_col * order_col, 0.0) / jnp.maximum(4.0 * (degree_f - 1.0) ** 2 - 1.0, 1.0))
        stepped = alpha_term * (cosine[None, :] * current - beta_term * before)
        at_start = order_ids[:, None] == degree
        past_start = order_ids[:, None] < degree
        fresh_value = jnp.where(at_start, 1.0, jnp.where(past_start, stepped, 0.0))
        fresh_log = jnp.where(at_start, start_log, scale_log)
        entry_value = fresh_value * jnp.exp(fresh_log)
        rescale = jnp.where(past_start | at_start, jnp.maximum(jnp.abs(fresh_value), jnp.abs(current)), 1.0)
        return ((current / rescale, fresh_value / rescale, fresh_log + jnp.log(rescale)), entry_value)
    degrees = jnp.arange(lat_count, dtype=jnp.int32)
    unused, legendre = lax.scan(advance, (blank_rows, blank_rows, blank_rows), degrees, unroll=16)
    return legendre

def filter_modes(banded, legendre, filter_block, quad_weights):
    coefficients = jnp.einsum('lmj,pmcj->pmcl', legendre, banded * quad_weights[None, None, None, :], precision=highest)
    coefficients = coefficients * filter_block[None, None, :, :]
    return jnp.einsum('lmj,pmcl->pmcj', legendre, coefficients, precision=highest)

def wrap_columns(extended):
    return jnp.concatenate([extended[:, :, -1:], extended, extended[:, :, :1]], axis=2)

def depthwise_core(extended, kernel, lat_rows, lon_cols):
    accumulated = jnp.zeros((extended.shape[0], lat_rows, lon_cols), jnp.float32)
    for row_shift in range(3):
        for col_shift in range(3):
            piece = extended[:, row_shift:row_shift + lat_rows, col_shift:col_shift + lon_cols].astype(jnp.float32)
            accumulated = accumulated + kernel[3 * row_shift + col_shift][:, None, None] * piece
    return accumulated.astype(jnp.bfloat16)

def channel_mlp(summed_low, norm_gain, weight_in, weight_out):
    summed = summed_low.astype(jnp.float32)
    scale_inv = lax.rsqrt(lax.optimization_barrier(jnp.mean(summed * summed, axis=0, keepdims=True)) + epsilon_norm)
    normed = (summed * scale_inv * norm_gain[:, None]).astype(jnp.bfloat16)
    hidden = lax.dot_general(weight_in, normed, (((0,), (0,)), ((), ())), preferred_element_type=jnp.float32)
    hidden = jax.nn.gelu(hidden, approximate=False).astype(jnp.bfloat16)
    result = summed + lax.dot_general(weight_out, hidden, (((0,), (0,)), ((), ())), preferred_element_type=jnp.float32)
    return result.astype(jnp.bfloat16)

def row_blocks(array):
    return jnp.transpose(array.reshape(C, N_LAT, LAT_DEV * NLON), (1, 0, 2))

def reference(latent_field, spectral_filter, conv_weight, norm_gain, weight_in, weight_out):
    chan_block = C // N_LON
    forward, inverse = fourier_tables(NLON, NLAT)
    legendre = legendre_rows(jnp.arange(NLAT, dtype=jnp.int32), NLAT)
    quad_weights = quadrature(NLAT)
    field_blocks = latent_field.reshape(N_LON, chan_block, NLAT, NLON)
    filter_blocks = spectral_filter.reshape(N_LON, chan_block, NLAT)
    kernel_blocks = jnp.transpose(conv_weight.reshape(9, N_LON, chan_block), (1, 0, 2))

    def branch_pair(inputs):
        field_block, filter_block, kernel_block = inputs
        flattened = field_block.astype(jnp.float32).reshape(chan_block * NLAT, NLON)
        spectrum = lax.dot_general(forward, flattened, (((1,), (1,)), ((), ())), precision=highest)
        spectrum = spectrum.reshape(2, NLAT, chan_block, NLAT)
        synthesized = filter_modes(spectrum, legendre, filter_block, quad_weights)
        regridded = lax.dot_general(synthesized.reshape(2 * NLAT, chan_block * NLAT), inverse, (((0,), (0,)), ((), ())), precision=highest)
        spectral = regridded.reshape(chan_block, NLAT, NLON).astype(jnp.bfloat16)
        extended = jnp.pad(field_block, ((0, 0), (1, 1), (0, 0)))
        local_mix = depthwise_core(wrap_columns(extended), kernel_block, NLAT, NLON)
        return (spectral, local_mix)
    spectral, local_mix = lax.map(branch_pair, (field_blocks, filter_blocks, kernel_blocks))
    spectral = spectral.reshape(C, NLAT, NLON)
    local_mix = local_mix.reshape(C, NLAT, NLON)

    def mix_band(inputs):
        field_band, spectral_band, conv_band = inputs
        summed = field_band.astype(jnp.float32) + spectral_band.astype(jnp.float32) + conv_band.astype(jnp.float32)
        return channel_mlp(summed.astype(jnp.bfloat16), norm_gain, weight_in, weight_out)
    bands = lax.map(mix_band, (row_blocks(latent_field), row_blocks(spectral), row_blocks(local_mix)))
    return jnp.transpose(bands, (1, 0, 2)).reshape(C, NLAT, NLON)
```

```python
import functools
import math

import jax
import jax.numpy as jnp
import numpy as np
from jax import lax
from jax.sharding import PartitionSpec as P

highest = lax.Precision.HIGHEST
epsilon_norm = 1e-06


def with_halo(cells, sides, width):
    for axis, dim in sides:
        count = lax.axis_size(axis)
        ends = count - 1
        head = lax.slice_in_dim(cells, 0, width, axis=dim)
        tail = lax.slice_in_dim(cells, cells.shape[dim] - width, cells.shape[dim], axis=dim)
        cells = jnp.concatenate(
            [
                lax.ppermute(tail, axis, [(i, (i + 1) % count) for i in range(ends)]),
                cells,
                lax.ppermute(head, axis, [((i + 1) % count, i) for i in range(ends)]),
            ],
            axis=dim,
        )
    return cells


def quadrature(lat_count):
    colatitude = (jnp.arange(lat_count, dtype=jnp.float32) + 0.5) * (math.pi / lat_count)
    return jnp.sin(colatitude) * (math.pi / lat_count)


def fourier_tables(lon_count, mode_count):
    wave_index = (
        jnp.arange(mode_count, dtype=jnp.int32)[:, None]
        * jnp.arange(lon_count, dtype=jnp.int32)[None, :]
    )
    phase_angle = (wave_index % lon_count).astype(jnp.float32) * (2.0 * math.pi / lon_count)
    cosine = jnp.cos(phase_angle)
    sine_table = jnp.sin(phase_angle)
    angle_step = 2.0 * math.pi / lon_count
    forward = jnp.concatenate([angle_step * cosine, -angle_step * sine_table], axis=0)
    weight = jnp.where(jnp.arange(mode_count, dtype=jnp.int32) == 0, 1.0, 2.0).astype(jnp.float32)[
        :, None
    ]
    inverse = jnp.concatenate([weight * cosine, -weight * sine_table], axis=0)
    return (forward, inverse)


def legendre_rows(order_ids, lat_count):
    colatitude = (jnp.arange(lat_count, dtype=jnp.float32) + 0.5) * (math.pi / lat_count)
    cosine = jnp.cos(colatitude)
    sine_col = jnp.sin(colatitude)
    order_f = order_ids.astype(jnp.float32)
    factor_index = jnp.arange(1, lat_count, dtype=jnp.float32)
    ratio_log = jnp.log((2.0 * factor_index - 1.0) / (2.0 * factor_index))
    included = (factor_index[None, :] <= order_f[:, None]).astype(jnp.float32)
    log_factor = jnp.sum(included * ratio_log[None, :], axis=1)
    start_log = 0.5 * jnp.log((2.0 * order_f + 1.0) / (4.0 * math.pi)) + 0.5 * log_factor
    start_log = start_log[:, None] + order_f[:, None] * jnp.log(sine_col)[None, :]
    blank_rows = jnp.zeros((order_ids.shape[0], lat_count), jnp.float32)
    order_col = order_f[:, None]

    def advance(state_carry, degree):
        before, current, scale_log = state_carry
        degree_f = degree.astype(jnp.float32)
        alpha_term = jnp.sqrt(
            (4.0 * degree_f * degree_f - 1.0)
            / jnp.maximum(degree_f * degree_f - order_col * order_col, 1.0)
        )
        beta_term = jnp.sqrt(
            jnp.maximum((degree_f - 1.0) ** 2 - order_col * order_col, 0.0)
            / jnp.maximum(4.0 * (degree_f - 1.0) ** 2 - 1.0, 1.0)
        )
        stepped = alpha_term * (cosine[None, :] * current - beta_term * before)
        at_start = order_ids[:, None] == degree
        past_start = order_ids[:, None] < degree
        fresh_value = jnp.where(at_start, 1.0, jnp.where(past_start, stepped, 0.0))
        fresh_log = jnp.where(at_start, start_log, scale_log)
        entry_value = fresh_value * jnp.exp(fresh_log)
        rescale = jnp.where(
            past_start | at_start, jnp.maximum(jnp.abs(fresh_value), jnp.abs(current)), 1.0
        )
        return (
            (current / rescale, fresh_value / rescale, fresh_log + jnp.log(rescale)),
            entry_value,
        )

    degrees = jnp.arange(lat_count, dtype=jnp.int32)
    unused, legendre = lax.scan(advance, (blank_rows, blank_rows, blank_rows), degrees)
    return legendre


def filter_modes(banded, legendre, filter_block, quad_weights):
    coefficients = jnp.einsum(
        "lmj,pmcj->pmcl", legendre, banded * quad_weights[None, None, None, :], precision=highest
    )
    coefficients = coefficients * filter_block[None, None, :, :]
    return jnp.einsum("lmj,pmcl->pmcj", legendre, coefficients, precision=highest)


def wrap_columns(extended):
    return jnp.concatenate([extended[:, :, -1:], extended, extended[:, :, :1]], axis=2)


def depthwise_core(extended, kernel, lat_rows, lon_cols):
    accumulated = jnp.zeros((extended.shape[0], lat_rows, lon_cols), jnp.float32)
    for row_shift in range(3):
        for col_shift in range(3):
            piece = extended[
                :, row_shift : row_shift + lat_rows, col_shift : col_shift + lon_cols
            ].astype(jnp.float32)
            accumulated = accumulated + kernel[3 * row_shift + col_shift][:, None, None] * piece
    return accumulated.astype(jnp.bfloat16)


def channel_mlp(summed_low, norm_gain, weight_in, weight_out):
    summed = summed_low.astype(jnp.float32)
    scale_inv = lax.rsqrt(jnp.mean(summed * summed, axis=0, keepdims=True) + epsilon_norm)
    normed = (summed * scale_inv * norm_gain[:, None]).astype(jnp.bfloat16)
    hidden = lax.dot_general(
        weight_in, normed, (((0,), (0,)), ((), ())), preferred_element_type=jnp.float32
    )
    hidden = jax.nn.gelu(hidden, approximate=False).astype(jnp.bfloat16)
    result = summed + lax.dot_general(
        weight_out, hidden, (((0,), (0,)), ((), ())), preferred_element_type=jnp.float32
    )
    return result.astype(jnp.bfloat16)


def add_three(first, second, third):
    total = first.astype(jnp.float32) + second.astype(jnp.float32) + third.astype(jnp.float32)
    return total.astype(jnp.bfloat16)


def on_device(latent_field, spectral_filter, conv_weight, norm_gain, weight_in, weight_out):
    channels, lat_rows, lon_cols = latent_field.shape
    sector_count = lax.axis_size("lon")
    lat_count = lat_rows * lax.axis_size("lat")
    lon_count = lon_cols * sector_count
    chan_block = channels // sector_count
    spread = lax.all_to_all(latent_field, "lon", split_axis=0, concat_axis=2, tiled=True)
    forward, inverse = fourier_tables(lon_count, lat_count)
    flattened = spread.astype(jnp.float32).reshape(chan_block * lat_rows, lon_count)
    spectrum = lax.dot_general(forward, flattened, (((1,), (1,)), ((), ())), precision=highest)
    spectrum = spectrum.reshape(2, lat_count, chan_block, lat_rows)
    banded = lax.all_to_all(spectrum, "lat", split_axis=1, concat_axis=3, tiled=True)
    order_ids = lax.axis_index("lat") * lat_rows + jnp.arange(lat_rows, dtype=jnp.int32)
    legendre = legendre_rows(order_ids, lat_count)
    synthesized = filter_modes(banded, legendre, spectral_filter, quadrature(lat_count))
    regathered = lax.all_to_all(synthesized, "lat", split_axis=3, concat_axis=1, tiled=True)
    regridded = lax.dot_general(
        regathered.reshape(2 * lat_count, chan_block * lat_rows),
        inverse,
        (((0,), (0,)), ((), ())),
        precision=highest,
    )
    spectral = regridded.reshape(chan_block, lat_rows, lon_count).astype(jnp.bfloat16)
    own_kernel = lax.dynamic_slice_in_dim(
        conv_weight, lax.axis_index("lon") * chan_block, chan_block, 1
    )
    rimmed = with_halo(spread, (("lat", 1),), 1)
    sector_mix = depthwise_core(wrap_columns(rimmed), own_kernel, lat_rows, lon_count)
    sector_sum = add_three(spread, spectral, sector_mix)
    summed = lax.all_to_all(sector_sum, "lon", split_axis=2, concat_axis=0, tiled=True)
    summed = summed.reshape(channels, lat_rows * lon_cols)
    result = channel_mlp(summed, norm_gain, weight_in, weight_out)
    return result.reshape(channels, lat_rows, lon_cols)


def transform_factors(lat_count, lon_count):
    theta = (np.arange(lat_count) + 0.5) * (math.pi / lat_count)
    x, s = np.cos(theta), np.sin(theta)
    quad = s * (math.pi / lat_count)
    phi = 2.0 * math.pi * np.arange(lon_count) / lon_count
    legendre, cosine, sine, degree, order = [], [], [], [], []
    for m in range(lat_count):
        k = np.arange(1, m + 1)
        log_start = 0.5 * (np.log((2 * m + 1) / (4 * math.pi)) + np.sum(np.log((2 * k - 1) / (2 * k))))
        before, current = np.zeros(lat_count), np.exp(log_start + m * np.log(s))
        for l in range(m, lat_count):
            if l > m:
                a = math.sqrt((4.0 * l * l - 1) / (l * l - m * m))
                b = math.sqrt(((l - 1.0) ** 2 - m * m) / (4.0 * (l - 1) ** 2 - 1))
                before, current = current, a * (x * current - b * before)
            legendre.append(current)
            cosine.append(np.cos(m * phi))
            sine.append(-np.sin(m * phi))
            degree.append(l)
            order.append(m)
    legendre = np.stack(legendre, 1)
    cosine, sine = np.stack(cosine, 1), np.stack(sine, 1)
    degree, order = np.array(degree), np.array(order)
    legendre = np.concatenate([legendre, legendre], 1)
    fourier = np.concatenate([cosine, sine], 1)
    weight = np.where(np.concatenate([order, order]) == 0, 1.0, 2.0)
    select = (np.arange(lat_count)[:, None] == np.concatenate([degree, degree])[None, :])
    forward = fourier * (2.0 * math.pi / lon_count)
    f32 = np.float32
    return (
        (legendre * quad[:, None]).astype(f32),
        forward.astype(f32),
        legendre.astype(f32),
        (fourier * weight).astype(f32),
        select.astype(f32),
    )


def full_table(rows, columns, lat_devices, lon_devices):
    width = rows.shape[1]
    rows = jnp.asarray(rows).reshape(lat_devices, 1, -1, 1, width)
    columns = jnp.asarray(columns).reshape(1, lon_devices, 1, -1, width)
    return (rows * columns).astype(jnp.bfloat16).reshape(-1, width)


def whole_sphere(lat_devices, lon_devices, latent_field, spectral_filter, conv_weight, norm_gain, weight_in, weight_out):
    channels, lat_rows, lon_cols = latent_field.shape
    devices = lat_devices * lon_devices
    lat_count, lon_count = lat_rows * lat_devices, lon_cols * lon_devices
    points = lat_rows * lon_cols
    own = channels // devices
    me_lat, me_lon = lax.axis_index("lat"), lax.axis_index("lon")
    start = (me_lat * lon_devices + me_lon) * own
    axes = ("lat", "lon")
    mine = lax.all_to_all(
        latent_field.reshape(devices, own, points), axes, split_axis=0, concat_axis=0, tiled=True
    )
    rows_f, cols_f, rows_i, cols_i, select = transform_factors(lat_count, lon_count)
    analysis = full_table(rows_f, cols_f, lat_devices, lon_devices)
    synthesis = full_table(rows_i, cols_i, lat_devices, lon_devices)
    filters = lax.all_gather(spectral_filter, "lon", axis=0, tiled=True)
    own_filter = lax.dynamic_slice_in_dim(filters, start, own, 0)
    gain = lax.dot_general(
        own_filter, jnp.asarray(select), (((1,), (0,)), ((), ())), precision=highest
    )
    flat = jnp.transpose(mine, (1, 0, 2)).reshape(own, devices * points)
    coefficients = lax.dot_general(
        flat, analysis, (((1,), (0,)), ((), ())), preferred_element_type=jnp.float32
    )
    coefficients = (coefficients * gain).astype(jnp.bfloat16)
    spectral = lax.dot_general(
        coefficients, synthesis, (((1,), (1,)), ((), ())), preferred_element_type=jnp.float32
    ).astype(jnp.bfloat16)
    spectral = spectral.reshape(own, lat_devices, lon_devices, lat_rows, lon_cols)
    own_kernel = lax.dynamic_slice_in_dim(conv_weight, start, own, 1)
    grid = flat.reshape(own, lat_devices, lon_devices, lat_rows, lon_cols)
    grid = jnp.transpose(grid, (0, 1, 3, 2, 4)).reshape(own, lat_count, lon_count)
    spectral = jnp.transpose(spectral, (0, 1, 3, 2, 4)).reshape(own, lat_count, lon_count)
    rimmed = jnp.pad(grid, ((0, 0), (1, 1), (0, 0)))
    mix = depthwise_core(wrap_columns(rimmed), own_kernel, lat_count, lon_count)
    total = add_three(grid, spectral, mix)
    total = total.reshape(own, lat_devices, lat_rows, lon_devices, lon_cols)
    total = jnp.transpose(total, (1, 3, 0, 2, 4)).reshape(devices, own, points)
    summed = lax.all_to_all(total, axes, split_axis=0, concat_axis=0, tiled=True)
    result = channel_mlp(summed.reshape(channels, points), norm_gain, weight_in, weight_out)
    return result.reshape(channels, lat_rows, lon_cols)


def whole_or_banded(lat_devices, lon_devices, *arguments):
    if arguments[0].shape[0] % (lat_devices * lon_devices) == 0:
        return whole_sphere(lat_devices, lon_devices, *arguments)
    return on_device(*arguments)


def solution(mesh):
    return jax.shard_map(
        functools.partial(whole_or_banded, mesh.shape["lat"], mesh.shape["lon"]),
        mesh=mesh,
        in_specs=(P(None, "lat", "lon"), P("lon", None), P(), P(), P(), P()),
        out_specs=P(None, "lat", "lon"),
        check_vma=False,
    )
```

```python
import functools
import math

import jax
import jax.numpy as jnp
import numpy as np
from jax import lax
from jax.experimental import pallas as pl
from jax.experimental.pallas import tpu as pltpu
from jax.sharding import PartitionSpec as P

highest = lax.Precision.HIGHEST
epsilon_norm = 1e-06


def with_halo(cells, sides, width):
    for axis, dim in sides:
        count = lax.axis_size(axis)
        ends = count - 1
        head = lax.slice_in_dim(cells, 0, width, axis=dim)
        tail = lax.slice_in_dim(cells, cells.shape[dim] - width, cells.shape[dim], axis=dim)
        cells = jnp.concatenate(
            [
                lax.ppermute(tail, axis, [(i, (i + 1) % count) for i in range(ends)]),
                cells,
                lax.ppermute(head, axis, [((i + 1) % count, i) for i in range(ends)]),
            ],
            axis=dim,
        )
    return cells


def quadrature(lat_count):
    colatitude = (jnp.arange(lat_count, dtype=jnp.float32) + 0.5) * (math.pi / lat_count)
    return jnp.sin(colatitude) * (math.pi / lat_count)


def fourier_tables(lon_count, mode_count):
    wave_index = (
        jnp.arange(mode_count, dtype=jnp.int32)[:, None]
        * jnp.arange(lon_count, dtype=jnp.int32)[None, :]
    )
    phase_angle = (wave_index % lon_count).astype(jnp.float32) * (2.0 * math.pi / lon_count)
    cosine = jnp.cos(phase_angle)
    sine_table = jnp.sin(phase_angle)
    angle_step = 2.0 * math.pi / lon_count
    forward = jnp.concatenate([angle_step * cosine, -angle_step * sine_table], axis=0)
    weight = jnp.where(jnp.arange(mode_count, dtype=jnp.int32) == 0, 1.0, 2.0).astype(jnp.float32)[
        :, None
    ]
    inverse = jnp.concatenate([weight * cosine, -weight * sine_table], axis=0)
    return (forward, inverse)


def legendre_rows(order_ids, lat_count):
    colatitude = (jnp.arange(lat_count, dtype=jnp.float32) + 0.5) * (math.pi / lat_count)
    cosine = jnp.cos(colatitude)
    sine_col = jnp.sin(colatitude)
    order_f = order_ids.astype(jnp.float32)
    factor_index = jnp.arange(1, lat_count, dtype=jnp.float32)
    ratio_log = jnp.log((2.0 * factor_index - 1.0) / (2.0 * factor_index))
    included = (factor_index[None, :] <= order_f[:, None]).astype(jnp.float32)
    log_factor = jnp.sum(included * ratio_log[None, :], axis=1)
    start_log = 0.5 * jnp.log((2.0 * order_f + 1.0) / (4.0 * math.pi)) + 0.5 * log_factor
    start_log = start_log[:, None] + order_f[:, None] * jnp.log(sine_col)[None, :]
    blank_rows = jnp.zeros((order_ids.shape[0], lat_count), jnp.float32)
    order_col = order_f[:, None]

    def advance(state_carry, degree):
        before, current, scale_log = state_carry
        degree_f = degree.astype(jnp.float32)
        alpha_term = jnp.sqrt(
            (4.0 * degree_f * degree_f - 1.0)
            / jnp.maximum(degree_f * degree_f - order_col * order_col, 1.0)
        )
        beta_term = jnp.sqrt(
            jnp.maximum((degree_f - 1.0) ** 2 - order_col * order_col, 0.0)
            / jnp.maximum(4.0 * (degree_f - 1.0) ** 2 - 1.0, 1.0)
        )
        stepped = alpha_term * (cosine[None, :] * current - beta_term * before)
        at_start = order_ids[:, None] == degree
        past_start = order_ids[:, None] < degree
        fresh_value = jnp.where(at_start, 1.0, jnp.where(past_start, stepped, 0.0))
        fresh_log = jnp.where(at_start, start_log, scale_log)
        entry_value = fresh_value * jnp.exp(fresh_log)
        rescale = jnp.where(
            past_start | at_start, jnp.maximum(jnp.abs(fresh_value), jnp.abs(current)), 1.0
        )
        return (
            (current / rescale, fresh_value / rescale, fresh_log + jnp.log(rescale)),
            entry_value,
        )

    degrees = jnp.arange(lat_count, dtype=jnp.int32)
    unused, legendre = lax.scan(advance, (blank_rows, blank_rows, blank_rows), degrees)
    return legendre


def filter_modes(banded, legendre, filter_block, quad_weights):
    coefficients = jnp.einsum(
        "lmj,pmcj->pmcl", legendre, banded * quad_weights[None, None, None, :], precision=highest
    )
    coefficients = coefficients * filter_block[None, None, :, :]
    return jnp.einsum("lmj,pmcl->pmcj", legendre, coefficients, precision=highest)


def wrap_columns(extended):
    return jnp.concatenate([extended[:, :, -1:], extended, extended[:, :, :1]], axis=2)


def depthwise_core(extended, kernel, lat_rows, lon_cols):
    accumulated = jnp.zeros((extended.shape[0], lat_rows, lon_cols), jnp.float32)
    for row_shift in range(3):
        for col_shift in range(3):
            piece = extended[
                :, row_shift : row_shift + lat_rows, col_shift : col_shift + lon_cols
            ].astype(jnp.float32)
            accumulated = accumulated + kernel[3 * row_shift + col_shift][:, None, None] * piece
    return accumulated.astype(jnp.bfloat16)


def channel_mlp(summed_low, norm_gain, weight_in, weight_out):
    summed = summed_low.astype(jnp.float32)
    scale_inv = lax.rsqrt(jnp.mean(summed * summed, axis=0, keepdims=True) + epsilon_norm)
    normed = (summed * scale_inv * norm_gain[:, None]).astype(jnp.bfloat16)
    hidden = lax.dot_general(
        weight_in, normed, (((0,), (0,)), ((), ())), preferred_element_type=jnp.float32
    )
    hidden = jax.nn.gelu(hidden, approximate=False).astype(jnp.bfloat16)
    result = summed + lax.dot_general(
        weight_out, hidden, (((0,), (0,)), ((), ())), preferred_element_type=jnp.float32
    )
    return result.astype(jnp.bfloat16)


def add_three(first, second, third):
    total = first.astype(jnp.float32) + second.astype(jnp.float32) + third.astype(jnp.float32)
    return total.astype(jnp.bfloat16)


def on_device(latent_field, spectral_filter, conv_weight, norm_gain, weight_in, weight_out):
    channels, lat_rows, lon_cols = latent_field.shape
    sector_count = lax.axis_size("lon")
    lat_count = lat_rows * lax.axis_size("lat")
    lon_count = lon_cols * sector_count
    chan_block = channels // sector_count
    spread = lax.all_to_all(latent_field, "lon", split_axis=0, concat_axis=2, tiled=True)
    forward, inverse = fourier_tables(lon_count, lat_count)
    flattened = spread.astype(jnp.float32).reshape(chan_block * lat_rows, lon_count)
    spectrum = lax.dot_general(forward, flattened, (((1,), (1,)), ((), ())), precision=highest)
    spectrum = spectrum.reshape(2, lat_count, chan_block, lat_rows)
    banded = lax.all_to_all(spectrum, "lat", split_axis=1, concat_axis=3, tiled=True)
    order_ids = lax.axis_index("lat") * lat_rows + jnp.arange(lat_rows, dtype=jnp.int32)
    legendre = legendre_rows(order_ids, lat_count)
    synthesized = filter_modes(banded, legendre, spectral_filter, quadrature(lat_count))
    regathered = lax.all_to_all(synthesized, "lat", split_axis=3, concat_axis=1, tiled=True)
    regridded = lax.dot_general(
        regathered.reshape(2 * lat_count, chan_block * lat_rows),
        inverse,
        (((0,), (0,)), ((), ())),
        precision=highest,
    )
    spectral = regridded.reshape(chan_block, lat_rows, lon_count).astype(jnp.bfloat16)
    own_kernel = lax.dynamic_slice_in_dim(
        conv_weight, lax.axis_index("lon") * chan_block, chan_block, 1
    )
    rimmed = with_halo(spread, (("lat", 1),), 1)
    sector_mix = depthwise_core(wrap_columns(rimmed), own_kernel, lat_rows, lon_count)
    sector_sum = add_three(spread, spectral, sector_mix)
    summed = lax.all_to_all(sector_sum, "lon", split_axis=2, concat_axis=0, tiled=True)
    summed = summed.reshape(channels, lat_rows * lon_cols)
    result = channel_mlp(summed, norm_gain, weight_in, weight_out)
    return result.reshape(channels, lat_rows, lon_cols)


def transform_table(lat_count, lon_count):
    theta = (np.arange(lat_count) + 0.5) * (math.pi / lat_count)
    x, s = np.cos(theta), np.sin(theta)
    phi = 2.0 * math.pi * np.arange(lon_count) / lon_count
    columns, degree, weight = [], [], []
    for m in range(lat_count):
        k = np.arange(1, m + 1)
        log_start = 0.5 * (
            np.log((2 * m + 1) / (4 * math.pi)) + np.sum(np.log((2 * k - 1) / (2 * k)))
        )
        before, current = np.zeros(lat_count), np.exp(log_start + m * np.log(s))
        for l in range(m, lat_count):
            if l > m:
                a = math.sqrt((4.0 * l * l - 1) / (l * l - m * m))
                b = math.sqrt(((l - 1.0) ** 2 - m * m) / (4.0 * (l - 1) ** 2 - 1))
                before, current = current, a * (x * current - b * before)
            for wave in [np.cos(m * phi), -np.sin(m * phi)][: 1 if m == 0 else 2]:
                columns.append((current[:, None] * wave[None, :]).reshape(-1))
                degree.append(l)
                weight.append(1.0 if m == 0 else 2.0)
    select = np.arange(lat_count)[:, None] == np.array(degree)[None, :]
    scaled = select * (np.array(weight) * (2.0 * math.pi / lon_count))[None, :]
    quad = np.repeat(s * (math.pi / lat_count), lon_count)
    return np.stack(columns, 1), scaled.astype(np.float32), quad.astype(np.float32)


def exchange_kernel(lat_devices, devices, src_ref, dst_ref, send_sem, recv_sem, local_sem):
    me = lax.axis_index("lon") * lat_devices + lax.axis_index("lat")

    def place(index):
        return (lax.rem(index, lat_devices), lax.div(index, lat_devices))

    barrier = pltpu.get_barrier_semaphore()

    def greet(step, carry):
        peer = lax.rem(me + step, devices)
        pl.semaphore_signal(
            barrier, inc=1, device_id=place(peer), device_id_type=pl.DeviceIdType.MESH
        )
        return carry

    lax.fori_loop(1, devices, greet, 0)
    kept = pltpu.make_async_copy(src_ref.at[me], dst_ref.at[me], local_sem)
    kept.start()
    pl.semaphore_wait(barrier, devices - 1)

    def copy(step, block, slot):
        return pltpu.make_async_remote_copy(
            src_ref=src_ref.at[block],
            dst_ref=dst_ref.at[slot],
            send_sem=send_sem.at[step],
            recv_sem=recv_sem.at[step],
            device_id=place(block),
            device_id_type=pl.DeviceIdType.MESH,
        )

    def send(step, carry):
        copy(step, lax.rem(me + step, devices), me).start()
        return carry

    def finish(step, carry):
        copy(step, lax.rem(me + step, devices), me).wait_send()
        source = lax.rem(me + devices - step, devices)
        copy(step, source, source).wait_recv()
        return carry

    lax.fori_loop(1, devices, send, 0)
    kept.wait()
    lax.fori_loop(1, devices, finish, 0)


def exchange(blocks, lat_devices, number):
    devices = blocks.shape[0]
    return pl.pallas_call(
        functools.partial(exchange_kernel, lat_devices, devices),
        out_shape=jax.ShapeDtypeStruct(blocks.shape, blocks.dtype),
        in_specs=[pl.BlockSpec(memory_space=pltpu.VMEM)],
        out_specs=pl.BlockSpec(memory_space=pltpu.VMEM),
        scratch_shapes=[
            pltpu.SemaphoreType.DMA((devices,)),
            pltpu.SemaphoreType.DMA((devices,)),
            pltpu.SemaphoreType.DMA,
        ],
        compiler_params=pltpu.CompilerParams(collective_id=number, has_side_effects=True),
        name=f"exchange_{number}",
    )(blocks)


def whole_sphere(lat_devices, lon_devices, latent_field, spectral_filter, conv_weight, norm_gain, weight_in, weight_out):
    channels, lat_rows, lon_cols = latent_field.shape
    devices = lat_devices * lon_devices
    lat_count, lon_count = lat_rows * lat_devices, lon_cols * lon_devices
    points = lat_rows * lon_cols
    own = channels // devices
    me_lat, me_lon = lax.axis_index("lat"), lax.axis_index("lon")
    packed = (devices, -1, math.gcd(own * points, 128))
    table, select, quad = transform_table(lat_count, lon_count)
    table = jnp.asarray(table.astype(jnp.bfloat16))
    mine = exchange(latent_field.reshape(packed), lat_devices, 0)
    own_filter = lax.dynamic_slice_in_dim(spectral_filter, me_lat * own, own, 0)
    gain = lax.dot_general(
        own_filter, jnp.asarray(select), (((1,), (0,)), ((), ())), precision=highest
    )
    grid = mine.reshape(lon_devices, lat_devices, own, lat_rows, lon_cols)
    grid = jnp.transpose(grid, (2, 1, 3, 0, 4)).reshape(own, lat_count, lon_count)
    flat = grid.reshape(own, lat_count * lon_count)
    weighted = (flat.astype(jnp.float32) * jnp.asarray(quad)[None, :]).astype(jnp.bfloat16)
    coefficients = lax.dot_general(
        weighted, table, (((1,), (0,)), ((), ())), preferred_element_type=jnp.float32
    )
    coefficients = (coefficients * gain).astype(jnp.bfloat16)
    spectral = lax.dot_general(
        coefficients, table, (((1,), (1,)), ((), ())), preferred_element_type=jnp.float32
    ).astype(jnp.bfloat16)
    spectral = spectral.reshape(own, lat_count, lon_count)
    start = (me_lon * lat_devices + me_lat) * own
    own_kernel = lax.dynamic_slice_in_dim(conv_weight, start, own, 1)
    rimmed = jnp.pad(grid, ((0, 0), (1, 1), (0, 0)))
    mix = depthwise_core(wrap_columns(rimmed), own_kernel, lat_count, lon_count)
    total = add_three(grid, spectral, mix)
    total = total.reshape(own, lat_devices, lat_rows, lon_devices, lon_cols)
    total = jnp.transpose(total, (3, 1, 0, 2, 4)).reshape(packed)
    summed = exchange(total, lat_devices, 1)
    result = channel_mlp(summed.reshape(channels, points), norm_gain, weight_in, weight_out)
    return result.reshape(channels, lat_rows, lon_cols)


def whole_or_banded(lat_devices, lon_devices, *arguments):
    if arguments[0].shape[0] % (lat_devices * lon_devices) == 0:
        return whole_sphere(lat_devices, lon_devices, *arguments)
    return on_device(*arguments)


def solution(mesh):
    return jax.shard_map(
        functools.partial(whole_or_banded, mesh.shape["lat"], mesh.shape["lon"]),
        mesh=mesh,
        in_specs=(P(None, "lat", "lon"), P("lon", None), P(), P(), P(), P()),
        out_specs=P(None, "lat", "lon"),
        check_vma=False,
    )
```

```python
import functools
import math

import jax
import jax.numpy as jnp
import numpy as np
from jax import lax
from jax.experimental import pallas as pl
from jax.experimental.pallas import tpu as pltpu
from jax.sharding import PartitionSpec as P

highest = lax.Precision.HIGHEST
epsilon_norm = 1e-06


def with_halo(cells, sides, width):
    for axis, dim in sides:
        count = lax.axis_size(axis)
        ends = count - 1
        head = lax.slice_in_dim(cells, 0, width, axis=dim)
        tail = lax.slice_in_dim(cells, cells.shape[dim] - width, cells.shape[dim], axis=dim)
        cells = jnp.concatenate(
            [
                lax.ppermute(tail, axis, [(i, (i + 1) % count) for i in range(ends)]),
                cells,
                lax.ppermute(head, axis, [((i + 1) % count, i) for i in range(ends)]),
            ],
            axis=dim,
        )
    return cells


def quadrature(lat_count):
    colatitude = (jnp.arange(lat_count, dtype=jnp.float32) + 0.5) * (math.pi / lat_count)
    return jnp.sin(colatitude) * (math.pi / lat_count)


def fourier_tables(lon_count, mode_count):
    wave_index = (
        jnp.arange(mode_count, dtype=jnp.int32)[:, None]
        * jnp.arange(lon_count, dtype=jnp.int32)[None, :]
    )
    phase_angle = (wave_index % lon_count).astype(jnp.float32) * (2.0 * math.pi / lon_count)
    cosine = jnp.cos(phase_angle)
    sine_table = jnp.sin(phase_angle)
    angle_step = 2.0 * math.pi / lon_count
    forward = jnp.concatenate([angle_step * cosine, -angle_step * sine_table], axis=0)
    weight = jnp.where(jnp.arange(mode_count, dtype=jnp.int32) == 0, 1.0, 2.0).astype(jnp.float32)[
        :, None
    ]
    inverse = jnp.concatenate([weight * cosine, -weight * sine_table], axis=0)
    return (forward, inverse)


def legendre_rows(order_ids, lat_count):
    colatitude = (jnp.arange(lat_count, dtype=jnp.float32) + 0.5) * (math.pi / lat_count)
    cosine = jnp.cos(colatitude)
    sine_col = jnp.sin(colatitude)
    order_f = order_ids.astype(jnp.float32)
    factor_index = jnp.arange(1, lat_count, dtype=jnp.float32)
    ratio_log = jnp.log((2.0 * factor_index - 1.0) / (2.0 * factor_index))
    included = (factor_index[None, :] <= order_f[:, None]).astype(jnp.float32)
    log_factor = jnp.sum(included * ratio_log[None, :], axis=1)
    start_log = 0.5 * jnp.log((2.0 * order_f + 1.0) / (4.0 * math.pi)) + 0.5 * log_factor
    start_log = start_log[:, None] + order_f[:, None] * jnp.log(sine_col)[None, :]
    blank_rows = jnp.zeros((order_ids.shape[0], lat_count), jnp.float32)
    order_col = order_f[:, None]

    def advance(state_carry, degree):
        before, current, scale_log = state_carry
        degree_f = degree.astype(jnp.float32)
        alpha_term = jnp.sqrt(
            (4.0 * degree_f * degree_f - 1.0)
            / jnp.maximum(degree_f * degree_f - order_col * order_col, 1.0)
        )
        beta_term = jnp.sqrt(
            jnp.maximum((degree_f - 1.0) ** 2 - order_col * order_col, 0.0)
            / jnp.maximum(4.0 * (degree_f - 1.0) ** 2 - 1.0, 1.0)
        )
        stepped = alpha_term * (cosine[None, :] * current - beta_term * before)
        at_start = order_ids[:, None] == degree
        past_start = order_ids[:, None] < degree
        fresh_value = jnp.where(at_start, 1.0, jnp.where(past_start, stepped, 0.0))
        fresh_log = jnp.where(at_start, start_log, scale_log)
        entry_value = fresh_value * jnp.exp(fresh_log)
        rescale = jnp.where(
            past_start | at_start, jnp.maximum(jnp.abs(fresh_value), jnp.abs(current)), 1.0
        )
        return (
            (current / rescale, fresh_value / rescale, fresh_log + jnp.log(rescale)),
            entry_value,
        )

    degrees = jnp.arange(lat_count, dtype=jnp.int32)
    unused, legendre = lax.scan(advance, (blank_rows, blank_rows, blank_rows), degrees)
    return legendre


def filter_modes(banded, legendre, filter_block, quad_weights):
    coefficients = jnp.einsum(
        "lmj,pmcj->pmcl", legendre, banded * quad_weights[None, None, None, :], precision=highest
    )
    coefficients = coefficients * filter_block[None, None, :, :]
    return jnp.einsum("lmj,pmcl->pmcj", legendre, coefficients, precision=highest)


def wrap_columns(extended):
    return jnp.concatenate([extended[:, :, -1:], extended, extended[:, :, :1]], axis=2)


def depthwise_core(extended, kernel, lat_rows, lon_cols):
    accumulated = jnp.zeros((extended.shape[0], lat_rows, lon_cols), jnp.float32)
    for row_shift in range(3):
        for col_shift in range(3):
            piece = extended[
                :, row_shift : row_shift + lat_rows, col_shift : col_shift + lon_cols
            ].astype(jnp.float32)
            accumulated = accumulated + kernel[3 * row_shift + col_shift][:, None, None] * piece
    return accumulated.astype(jnp.bfloat16)


def channel_mlp(summed_low, norm_gain, weight_in, weight_out):
    summed = summed_low.astype(jnp.float32)
    scale_inv = lax.rsqrt(jnp.mean(summed * summed, axis=0, keepdims=True) + epsilon_norm)
    normed = (summed * scale_inv * norm_gain[:, None]).astype(jnp.bfloat16)
    hidden = lax.dot_general(
        weight_in, normed, (((0,), (0,)), ((), ())), preferred_element_type=jnp.float32
    )
    hidden = jax.nn.gelu(hidden, approximate=False).astype(jnp.bfloat16)
    result = summed + lax.dot_general(
        weight_out, hidden, (((0,), (0,)), ((), ())), preferred_element_type=jnp.float32
    )
    return result.astype(jnp.bfloat16)


def add_three(first, second, third):
    total = first.astype(jnp.float32) + second.astype(jnp.float32) + third.astype(jnp.float32)
    return total.astype(jnp.bfloat16)


def on_device(latent_field, spectral_filter, conv_weight, norm_gain, weight_in, weight_out):
    channels, lat_rows, lon_cols = latent_field.shape
    sector_count = lax.axis_size("lon")
    lat_count = lat_rows * lax.axis_size("lat")
    lon_count = lon_cols * sector_count
    chan_block = channels // sector_count
    spread = lax.all_to_all(latent_field, "lon", split_axis=0, concat_axis=2, tiled=True)
    forward, inverse = fourier_tables(lon_count, lat_count)
    flattened = spread.astype(jnp.float32).reshape(chan_block * lat_rows, lon_count)
    spectrum = lax.dot_general(forward, flattened, (((1,), (1,)), ((), ())), precision=highest)
    spectrum = spectrum.reshape(2, lat_count, chan_block, lat_rows)
    banded = lax.all_to_all(spectrum, "lat", split_axis=1, concat_axis=3, tiled=True)
    order_ids = lax.axis_index("lat") * lat_rows + jnp.arange(lat_rows, dtype=jnp.int32)
    legendre = legendre_rows(order_ids, lat_count)
    synthesized = filter_modes(banded, legendre, spectral_filter, quadrature(lat_count))
    regathered = lax.all_to_all(synthesized, "lat", split_axis=3, concat_axis=1, tiled=True)
    regridded = lax.dot_general(
        regathered.reshape(2 * lat_count, chan_block * lat_rows),
        inverse,
        (((0,), (0,)), ((), ())),
        precision=highest,
    )
    spectral = regridded.reshape(chan_block, lat_rows, lon_count).astype(jnp.bfloat16)
    own_kernel = lax.dynamic_slice_in_dim(
        conv_weight, lax.axis_index("lon") * chan_block, chan_block, 1
    )
    rimmed = with_halo(spread, (("lat", 1),), 1)
    sector_mix = depthwise_core(wrap_columns(rimmed), own_kernel, lat_rows, lon_count)
    sector_sum = add_three(spread, spectral, sector_mix)
    summed = lax.all_to_all(sector_sum, "lon", split_axis=2, concat_axis=0, tiled=True)
    summed = summed.reshape(channels, lat_rows * lon_cols)
    result = channel_mlp(summed, norm_gain, weight_in, weight_out)
    return result.reshape(channels, lat_rows, lon_cols)


def arrival_order(grid, lon_devices):
    return grid.reshape(grid.shape[0], lon_devices, -1).transpose(1, 0, 2).reshape(-1)


def transform_table(lat_count, lon_count, lon_devices):
    theta = (np.arange(lat_count) + 0.5) * (math.pi / lat_count)
    x, s = np.cos(theta), np.sin(theta)
    phi = 2.0 * math.pi * np.arange(lon_count) / lon_count
    columns, degree, weight = [], [], []
    for m in range(lat_count):
        k = np.arange(1, m + 1)
        log_start = 0.5 * (
            np.log((2 * m + 1) / (4 * math.pi)) + np.sum(np.log((2 * k - 1) / (2 * k)))
        )
        before, current = np.zeros(lat_count), np.exp(log_start + m * np.log(s))
        for l in range(m, lat_count):
            if l > m:
                a = math.sqrt((4.0 * l * l - 1) / (l * l - m * m))
                b = math.sqrt(((l - 1.0) ** 2 - m * m) / (4.0 * (l - 1) ** 2 - 1))
                before, current = current, a * (x * current - b * before)
            for wave in [np.cos(m * phi), -np.sin(m * phi)][: 1 if m == 0 else 2]:
                columns.append(arrival_order(current[:, None] * wave[None, :], lon_devices))
                degree.append(l)
                weight.append(1.0 if m == 0 else 2.0)
    select = np.arange(lat_count)[:, None] == np.array(degree)[None, :]
    scaled = select * (np.array(weight) * (2.0 * math.pi / lon_count))[None, :]
    quad = np.broadcast_to((s * (math.pi / lat_count))[:, None], (lat_count, lon_count))
    quad = arrival_order(quad, lon_devices)
    return np.stack(columns, 1), scaled.astype(np.float32), quad.astype(np.float32)


def exchange_kernel(lat_devices, devices, src_ref, dst_ref, send_sem, recv_sem, local_sem):
    me = lax.axis_index("lon") * lat_devices + lax.axis_index("lat")

    def place(index):
        return (lax.rem(index, lat_devices), lax.div(index, lat_devices))

    barrier = pltpu.get_barrier_semaphore()

    def greet(step, carry):
        peer = lax.rem(me + step, devices)
        pl.semaphore_signal(
            barrier, inc=1, device_id=place(peer), device_id_type=pl.DeviceIdType.MESH
        )
        return carry

    lax.fori_loop(1, devices, greet, 0)
    kept = pltpu.make_async_copy(src_ref.at[me], dst_ref.at[me], local_sem)
    kept.start()
    pl.semaphore_wait(barrier, devices - 1)

    def copy(step, block, slot):
        return pltpu.make_async_remote_copy(
            src_ref=src_ref.at[block],
            dst_ref=dst_ref.at[slot],
            send_sem=send_sem.at[step],
            recv_sem=recv_sem.at[step],
            device_id=place(block),
            device_id_type=pl.DeviceIdType.MESH,
        )

    def send(step, carry):
        copy(step, lax.rem(me + step, devices), me).start()
        return carry

    def finish(step, carry):
        copy(step, lax.rem(me + step, devices), me).wait_send()
        source = lax.rem(me + devices - step, devices)
        copy(step, source, source).wait_recv()
        return carry

    lax.fori_loop(1, devices, send, 0)
    kept.wait()
    lax.fori_loop(1, devices, finish, 0)


def exchange(blocks, lat_devices, number):
    devices = blocks.shape[0]
    return pl.pallas_call(
        functools.partial(exchange_kernel, lat_devices, devices),
        out_shape=jax.ShapeDtypeStruct(blocks.shape, blocks.dtype),
        in_specs=[pl.BlockSpec(memory_space=pltpu.VMEM)],
        out_specs=pl.BlockSpec(memory_space=pltpu.VMEM),
        scratch_shapes=[
            pltpu.SemaphoreType.DMA((devices,)),
            pltpu.SemaphoreType.DMA((devices,)),
            pltpu.SemaphoreType.DMA,
        ],
        compiler_params=pltpu.CompilerParams(collective_id=number, has_side_effects=True),
        name=f"exchange_{number}",
    )(blocks)


def sphere_kernel(lat_count, lon_cols, flat_ref, quad_ref, table_ref, gain_ref, taps_ref, out_ref):
    count = flat_ref.shape[1]
    low = flat_ref[...]
    field = low.astype(jnp.float32)
    weighted = (field * quad_ref[...]).astype(jnp.bfloat16)
    table = table_ref[...]
    coefficients = jnp.dot(weighted, table, preferred_element_type=jnp.float32)
    coefficients = (coefficients * gain_ref[...]).astype(jnp.bfloat16)
    spectral = lax.dot_general(
        coefficients, table, (((1,), (1,)), ((), ())), preferred_element_type=jnp.float32
    )
    point = lax.broadcasted_iota(jnp.int32, field.shape, 1)
    column = lax.rem(point, lon_cols)
    row = lax.rem(lax.div(point, lon_cols), lat_count)
    jump = lat_count * lon_cols - (lon_cols - 1)
    west = jnp.where(column == 0, pltpu.roll(field, jump, 1), pltpu.roll(field, 1, 1))
    east = jnp.where(
        column == lon_cols - 1, pltpu.roll(field, count - jump, 1), pltpu.roll(field, count - 1, 1)
    )
    taps = taps_ref[...]

    def mixed(shift):
        return (
            taps[:, 3 * shift : 3 * shift + 1] * west
            + taps[:, 3 * shift + 1 : 3 * shift + 2] * field
            + taps[:, 3 * shift + 2 : 3 * shift + 3] * east
        )

    north = jnp.where(row == 0, 0.0, pltpu.roll(mixed(0), lon_cols, 1))
    south = jnp.where(row == lat_count - 1, 0.0, pltpu.roll(mixed(2), count - lon_cols, 1))
    mix = (north + mixed(1) + south).astype(jnp.bfloat16).astype(jnp.float32)
    spectral = spectral.astype(jnp.bfloat16).astype(jnp.float32)
    out_ref[...] = (field + spectral + mix).astype(jnp.bfloat16)


def whole_sphere(lat_devices, lon_devices, latent_field, spectral_filter, conv_weight, norm_gain, weight_in, weight_out):
    channels, lat_rows, lon_cols = latent_field.shape
    devices = lat_devices * lon_devices
    lat_count, lon_count = lat_rows * lat_devices, lon_cols * lon_devices
    points = lat_rows * lon_cols
    own = channels // devices
    padding = ((0, -own % 16), (0, 0))
    me_lat, me_lon = lax.axis_index("lat"), lax.axis_index("lon")
    packed = (devices, -1, math.gcd(own * points, 128))
    table, select, quad = transform_table(lat_count, lon_count, lon_devices)
    table = jnp.asarray(table.astype(jnp.bfloat16))
    own_filter = lax.dynamic_slice_in_dim(spectral_filter, me_lat * own, own, 0)
    gain = lax.dot_general(
        own_filter, jnp.asarray(select), (((1,), (0,)), ((), ())), precision=highest
    )
    start = (me_lon * lat_devices + me_lat) * own
    taps = lax.dynamic_slice_in_dim(conv_weight, start, own, 1).T
    mine = exchange(latent_field.reshape(packed), lat_devices, 0)
    flat = jnp.transpose(mine.reshape(devices, own, points), (1, 0, 2)).reshape(own, -1)
    total = pl.pallas_call(
        functools.partial(sphere_kernel, lat_count, lon_cols),
        out_shape=jax.ShapeDtypeStruct((own + padding[0][1], devices * points), jnp.bfloat16),
        in_specs=[pl.BlockSpec(memory_space=pltpu.VMEM)] * 5,
        out_specs=pl.BlockSpec(memory_space=pltpu.VMEM),
        name="sphere",
    )(jnp.pad(flat, padding), jnp.asarray(quad)[None, :], table, jnp.pad(gain, padding), jnp.pad(taps, padding))
    total = jnp.transpose(total[:own].reshape(own, devices, points), (1, 0, 2))
    summed = exchange(total.reshape(packed), lat_devices, 1)
    result = channel_mlp(summed.reshape(channels, points), norm_gain, weight_in, weight_out)
    return result.reshape(channels, lat_rows, lon_cols)


def whole_or_banded(lat_devices, lon_devices, *arguments):
    if arguments[0].shape[0] % (lat_devices * lon_devices) == 0:
        return whole_sphere(lat_devices, lon_devices, *arguments)
    return on_device(*arguments)


def solution(mesh):
    return jax.shard_map(
        functools.partial(whole_or_banded, mesh.shape["lat"], mesh.shape["lon"]),
        mesh=mesh,
        in_specs=(P(None, "lat", "lon"), P("lon", None), P(), P(), P(), P()),
        out_specs=P(None, "lat", "lon"),
        check_vma=False,
    )
```
